8 devices in a mesh: data: 1 (over z), store: 2 (over y), model: 4 (over x, core).
Axes of the slice: x: 2, y: 2, z: 1, core: 2. Of those that a mesh axis runs over, the one named last changes fastest.
Arguments:
- queries: bfloat16 [64, 2048], P('data')
- w_head: bfloat16 [2048, 256000], P(None, 'model')
- store_keys: bfloat16 [65536, 2048], P(('store', 'model'))
- store_tok: int32 [65536], P(('store', 'model'))
- temperature: float32 [], replicated
- mix_weight: float32 [], replicated
Outputs:
- output: float32 [64, 256000], P(('data', 'store'), 'model')
All inputs are finite; a program needn't handle non-finite values.
Results may differ from the reference program's by a relative error of at most 0.001.
Values are sent between devices in bfloat16 or wider.
A program may use at most 1.25 GiB of HBM per device.

```python
import jax
import jax.numpy as jnp
from jax import lax

HIDDEN = 2048
VOCAB = 256000
ROWS_DEV = 32
KEYS_DEV = 8192
STORE_DEVS = 2
MODEL_DEVS = 4
BATCH = ROWS_DEV * STORE_DEVS
SHARDS = STORE_DEVS * MODEL_DEVS
N_KEYS = KEYS_DEV * SHARDS


def setup_inputs(seed: int = 0, part: int = 0) -> dict:
    base_key = jax.random.key(seed)
    part_key = jax.random.fold_in(base_key, part)
    key_head, key_store, key_tok_a, key_tok_b, key_temp, key_mix = jax.random.split(base_key, 6)
    queries = jax.random.normal(part_key, (BATCH, HIDDEN), jnp.float32)
    w_head = jax.random.normal(key_head, (HIDDEN, VOCAB), jnp.float32) * HIDDEN ** -0.5
    store_keys = jax.random.normal(key_store, (N_KEYS, HIDDEN), jnp.float32)
    tok_a = jax.random.randint(key_tok_a, (N_KEYS,), 0, VOCAB, jnp.int32)
    tok_b = jax.random.randint(key_tok_b, (N_KEYS,), 0, VOCAB, jnp.int32)
    store_tok = jnp.minimum(tok_a, tok_b).at[0].set(0).at[N_KEYS - 1].set(VOCAB - 1)
    temperature = (6.0 * HIDDEN) ** 0.5 / 1.5 * jax.random.uniform(key_temp, (), jnp.float32, minval=0.6, maxval=1.5)
    mix_weight = jax.random.uniform(key_mix, (), jnp.float32, minval=0.25, maxval=0.5)
    return {"queries": queries.astype(jnp.bfloat16), "w_head": w_head.astype(jnp.bfloat16), "store_keys": store_keys.astype(jnp.bfloat16), "store_tok": store_tok, "temperature": temperature, "mix_weight": mix_weight}


def reference(queries, w_head, store_keys, store_tok, temperature, mix_weight):
    key_blocks = store_keys.reshape(SHARDS, KEYS_DEV, HIDDEN)
    tok_blocks = store_tok.reshape(SHARDS, KEYS_DEV)

    def block_scores(block):
        key_dots = jnp.dot(block, queries.T, preferred_element_type=jnp.float32)
        key_norms = jnp.sum(jnp.square(block.astype(jnp.float32)), axis=1)
        return (2.0 * key_dots - key_norms[:, None]) / temperature

    block_top = lax.map(lambda block: jnp.max(block_scores(block), axis=0), key_blocks)
    row_top = jnp.max(block_top, axis=0)

    def accumulate(carry, pair):
        histogram, row_total = carry
        block, tok_ids = pair
        weights = jnp.exp(block_scores(block) - row_top)
        histogram = histogram + jax.ops.segment_sum(weights, tok_ids, num_segments=VOCAB)
        row_total = row_total + jnp.sum(weights, axis=0)
        return (histogram, row_total), None

    init_state = (jnp.zeros((VOCAB, BATCH), jnp.float32), jnp.zeros((BATCH,), jnp.float32))
    (histogram, row_total), _ = lax.scan(accumulate, init_state, (key_blocks, tok_blocks))
    knn_prob = (histogram / row_total).T
    logits = jnp.dot(queries, w_head, preferred_element_type=jnp.float32)
    lm_exp = jnp.exp(logits - jnp.max(logits, axis=1, keepdims=True))
    lm_prob = lm_exp / jnp.sum(lm_exp, axis=1, keepdims=True)
    return jnp.log(mix_weight * knn_prob + (1.0 - mix_weight) * lm_prob)
```

```python
import functools

import jax
import jax.numpy as jnp
from jax import lax
from jax.experimental import pallas as pl
from jax.experimental.pallas import tpu as pltpu
from jax.sharding import PartitionSpec as P

MESH = pl.DeviceIdType.MESH
F32, BF16, I32 = jnp.float32, jnp.bfloat16, jnp.int32
VLIM = 60 * 1024 * 1024
CHUNK = 32


def iota(shape, dim):
    return lax.broadcasted_iota(I32, shape, dim)


def sort_rows(x):
    n = x.shape[0] * 128
    pos = iota(x.shape, 0) * 128 + iota(x.shape, 1)
    k = 2
    while k <= n:
        j = k // 2
        while j >= 1:
            if j >= 128:
                ahead, behind = pltpu.roll(x, 64 - j // 128, 0), pltpu.roll(x, j // 128, 0)
            else:
                ahead, behind = pltpu.roll(x, 128 - j, 1), pltpu.roll(x, j, 1)
            first = (pos & j) == 0
            other = jnp.where(first, ahead, behind)
            low = ((pos & k) == 0) == first
            x = jnp.where(low, jnp.minimum(x, other), jnp.maximum(x, other))
            j //= 2
        k *= 2
    return x


def score_kernel(qt_ref, keys_ref, tok_ref, tau_ref, e_ref, tok_out, start_out, stat_out, s_ref, top_ref, perm_v, perm_s, hot_a, hot_b, rows_ref, sem):
    step, steps = pl.program_id(0), pl.num_programs(0)
    kb = keys_ref.shape[0]
    sub = 256

    @pl.when(step == 0)
    def _():
        top_ref[...] = jnp.full_like(top_ref, -jnp.inf)
        tok = tok_ref[...]
        packed = sort_rows(tok * 8192 + (iota((64, 128), 0) * 128 + iota((64, 128), 1)))
        tok_out[...] = packed >> 13
        perm_v[...] = packed & 8191
        cp = pltpu.make_async_copy(perm_v, perm_s, sem)
        cp.start()
        for r in range(64):
            tile = tok_ref[r : r + 1, :] >> 8
            lanes = slice(r * 128, (r + 1) * 128)
            hot_a[:, lanes] = jnp.where(iota((32, 128), 0) == (tile >> 5), 1.0, 0.0).astype(BF16)
            hot_b[:, lanes] = jnp.where(iota((128, 128), 0) == (tile & 31), 1.0, 0.0).astype(BF16)
        cnt = lax.dot_general(hot_a[...], hot_b[...], (((1,), (1,)), ((), ())), preferred_element_type=F32)
        inc = cnt
        for sh in (1, 2, 4, 8, 16):
            inc = inc + jnp.where(iota((32, 128), 1) >= sh, pltpu.roll(inc, sh, 1), 0.0)
        tot = jnp.broadcast_to(jnp.sum(cnt, axis=1, keepdims=True), (32, 128))
        rp = tot
        for sh in (1, 2, 4, 8, 16):
            rp = rp + jnp.where(iota((32, 128), 0) >= sh, pltpu.roll(rp, sh, 0), 0.0)
        start_out[...] = ((inc - cnt) + (rp - tot)).astype(I32)
        cp.wait()

    def score(i, _):
        at = pl.multiple_of(i * sub, sub)
        kv = keys_ref[pl.ds(at, sub), :]
        dots = jnp.dot(kv, qt_ref[...], preferred_element_type=F32)
        kf = kv.astype(F32)
        norm = jnp.sum(kf * kf, axis=1, keepdims=True)
        s = (2.0 * dots - norm) / tau_ref[0, 0]
        s_ref[pl.ds(pl.multiple_of(step * kb + at, sub), sub), :] = s
        top_ref[...] = jnp.maximum(top_ref[...], jnp.max(s.reshape(sub // 8, 8, 128), axis=0))
        return 0

    lax.fori_loop(0, kb // sub, score, 0)

    @pl.when(step == steps - 1)
    def _():
        top = jnp.max(top_ref[...], axis=0, keepdims=True)

        def block(b, total):
            for u in range(128):
                rows_ref[u : u + 1, :] = s_ref[pl.ds(perm_s[b, u], 1), :]
            x = jnp.exp(rows_ref[...] - top)
            total = total + jnp.sum(x.reshape(16, 8, 128), axis=0)
            xt = x.T
            lanes = pl.ds(pl.multiple_of(b * 128, 128), 128)
            for g in range(8):
                e_ref[g // 4, g % 4, :, lanes] = xt[8 * g : 8 * g + 8, :]
            return total

        total = lax.fori_loop(0, 64, block, jnp.zeros((8, 128), F32))
        total = jnp.sum(total, axis=0, keepdims=True)
        mt = jnp.broadcast_to(top, (128, 128)).T
        zt = jnp.broadcast_to(total, (128, 128)).T
        for s in range(2):
            stat_out[s, 0] = mt[32 * s : 32 * s + 32]
            stat_out[s, 1] = zt[32 * s : 32 * s + 32]


def scores(qt, keys, tok, tau, kb=1024):
    n = keys.shape[0]
    whole = lambda *s: pl.BlockSpec(s, lambda i: (0,) * len(s))
    return pl.pallas_call(
        score_kernel,
        grid=(n // kb,),
        in_specs=[whole(2048, 128), pl.BlockSpec((kb, 2048), lambda i: (i, 0)), whole(64, 128), pl.BlockSpec(memory_space=pltpu.SMEM)],
        out_specs=[whole(2, 4, 8, n), whole(64, 128), whole(32, 128), whole(2, 2, 32, 128)],
        out_shape=[jax.ShapeDtypeStruct((2, 4, 8, n), F32), jax.ShapeDtypeStruct((64, 128), I32), jax.ShapeDtypeStruct((32, 128), I32), jax.ShapeDtypeStruct((2, 2, 32, 128), F32)],
        scratch_shapes=[
            pltpu.VMEM((n, 128), F32), pltpu.VMEM((8, 128), F32), pltpu.VMEM((64, 128), I32), pltpu.SMEM((64, 128), I32),
            pltpu.VMEM((32, n), BF16), pltpu.VMEM((128, n), BF16), pltpu.VMEM((128, 128), F32), pltpu.SemaphoreType.DMA,
        ],
        compiler_params=pltpu.CompilerParams(vmem_limit_bytes=VLIM),
        name="scores",
    )(qt, keys, tok, tau)


def peers():
    s, m = lax.axis_index("store"), lax.axis_index("model")
    x, c = m // 2, m % 2
    return s, m, 1 - s, (1 - x) * 2 + c, x * 2 + (1 - c)


def remote(src, dst, ss, rs, s, m):
    return pltpu.make_async_remote_copy(src_ref=src, dst_ref=dst, send_sem=ss, recv_sem=rs, device_id=(0, s, m), device_id_type=MESH)


def exchange_kernel(e_ref, tok_ref, start_ref, stat_ref, e_all, tok_all, start_all, stat_all, es, er, ps, pr, ts, tr):
    s, m, so, mx, mc = peers()
    me = s * 4 + m
    barrier = pltpu.get_barrier_semaphore()
    for j in range(1, 8):
        d = lax.rem(me + j, 8)
        pl.semaphore_signal(barrier, inc=1, device_id=(0, d // 4, lax.rem(d, 4)), device_id_type=MESH)
    pl.semaphore_wait(barrier, 7)

    small = []
    for j in range(1, 8):
        d = lax.rem(me + j, 8)
        ds_, dm = d // 4, lax.rem(d, 4)
        for k, (a, b) in enumerate(((tok_ref, tok_all.at[me]), (start_ref, start_all.at[me]), (stat_ref.at[ds_], stat_all.at[me]))):
            small.append(remote(a, b, ts.at[j, k], tr.at[j, k], ds_, dm))
    for c in small:
        c.start()
    far = []
    for r in range(4):
        far.append([
            remote(e_ref.at[so, r], e_all.at[me, r], es.at[0, r], er.at[0, r], so, mx),
            remote(e_ref.at[s, r], e_all.at[me, r], es.at[1, r], er.at[1, r], s, mx),
            remote(e_ref.at[so, r], e_all.at[me, r], es.at[2, r], er.at[2, r], so, m),
        ])
        for c in far[-1]:
            c.start()
    own = [remote(e_ref.at[s, r], e_all.at[me, r], ps.at[3, r], pr.at[3, r], s, mc) for r in range(4)]
    for c in own:
        c.start()
    came = (so * 4 + mx, s * 4 + mx, so * 4 + m)
    fwd = []
    for r in range(4):
        for k in (1, 2, 0):
            far[r][k].wait_recv()
            f = remote(e_all.at[came[k], r], e_all.at[came[k], r], ps.at[k, r], pr.at[k, r], s, mc)
            f.start()
            fwd.append(f)
    for c in own + fwd:
        c.wait()
    for r in range(4):
        for c in far[r]:
            c.wait_send()
    for c in small:
        c.wait()


def exchange(e, tok, start, stat):
    n = e.shape[-1]
    anyspec = pl.BlockSpec(memory_space=pl.ANY)
    return pl.pallas_call(
        exchange_kernel,
        in_specs=[anyspec] * 4,
        out_specs=[anyspec] * 4,
        out_shape=[jax.ShapeDtypeStruct((8, 4, 8, n), F32), jax.ShapeDtypeStruct((8, 64, 128), I32), jax.ShapeDtypeStruct((8, 32, 128), I32), jax.ShapeDtypeStruct((8, 2, 32, 128), F32)],
        scratch_shapes=[
            pltpu.SemaphoreType.DMA((3, 4)), pltpu.SemaphoreType.DMA((3, 4)), pltpu.SemaphoreType.DMA((4, 4)), pltpu.SemaphoreType.DMA((4, 4)),
            pltpu.SemaphoreType.DMA((8, 3)), pltpu.SemaphoreType.DMA((8, 3)),
        ],
        compiler_params=pltpu.CompilerParams(collective_id=0, has_side_effects=True),
        name="exchange",
    )(e, tok, start, stat)


def piece(e_ref, tok_ref, scale, starts, ends, base):
    lane = iota((32, 128), 1)
    lane1 = iota((1, 128), 1)
    halves, toks = [], []
    for h in range(2):
        acc, tacc = None, None
        for i in range(4):
            d = 4 * h + i
            at = starts[d]
            row, off = jnp.minimum(at >> 7, 63), at & 127
            nxt = jnp.minimum(row + 1, 63)
            v0 = e_ref[d, :, pl.ds(pl.multiple_of(row * 128, 128), 128)]
            v1 = e_ref[d, :, pl.ds(pl.multiple_of(nxt * 128, 128), 128)]
            sh = (CHUNK * i - off) & 127
            v = pltpu.roll(jnp.where(lane >= off, v0, v1), sh, 1)
            t0, t1 = tok_ref[d, pl.ds(row, 1), :], tok_ref[d, pl.ds(nxt, 1), :]
            t = pltpu.roll(jnp.where(lane1 >= off, t0, t1), sh, 1)
            t = jnp.where(lane1 - CHUNK * i < ends[d] - at, t, -1)
            if i == 0:
                acc, tacc = v, t
            else:
                acc = jnp.where(lane >= CHUNK * i, v, acc)
                tacc = jnp.where(lane1 >= CHUNK * i, t, tacc)
        halves.append(acc)
        toks.append(tacc)
    e = jnp.concatenate(halves, axis=1) * scale
    tok = jnp.concatenate(toks, axis=1) - base
    hi = e.astype(BF16)
    rest = e - hi.astype(F32)
    mid = rest.astype(BF16)
    low = (rest - mid.astype(F32)).astype(BF16)
    lhs = jnp.concatenate([hi, mid, low], axis=0)
    hot = jnp.where(iota((256, 256), 0) == tok, 1.0, 0.0).astype(BF16)
    out = lax.dot_general(lhs, hot, (((1,), (1,)), ((), ())), preferred_element_type=F32)
    return out[0:32] + out[32:64] + out[64:96]


def head_hist_kernel(per, start_s, base_s, q_ref, w_ref, e_ref, tok_ref, scale_ref, logit_ref, hist_ref, stat_ref, top_ref, sum_ref):
    step, steps = pl.program_id(0), pl.num_programs(0)

    @pl.when(step == 0)
    def _():
        top_ref[...] = jnp.full_like(top_ref, -jnp.inf)
        sum_ref[...] = jnp.zeros_like(sum_ref)

    logits = jnp.dot(q_ref[...], w_ref[...], preferred_element_type=F32)
    logit_ref[...] = logits
    old = top_ref[...]
    new = jnp.maximum(old, jnp.max(logits, axis=1, keepdims=True))
    sum_ref[...] = sum_ref[...] * jnp.exp(old - new) + jnp.sum(jnp.exp(logits - new[:, 0:1]), axis=1, keepdims=True)
    top_ref[...] = new
    scale = scale_ref[...]
    for i in range(per):
        t = step * per + i
        starts = [start_s[d, t] for d in range(8)]
        ends = [start_s[d, t + 1] for d in range(8)]
        base = base_s[0] + t * 256
        cols = slice(i * 256, (i + 1) * 256)
        hist_ref[:, cols] = piece(e_ref, tok_ref, scale, starts, ends, base)
        most = functools.reduce(jnp.maximum, [b - a for a, b in zip(starts, ends)])

        @pl.when(most > CHUNK)
        def _():
            def more(it, _):
                at = [jnp.minimum(a + it * CHUNK, b) for a, b in zip(starts, ends)]
                hist_ref[:, cols] += piece(e_ref, tok_ref, scale, at, ends, base)
                return 0

            lax.fori_loop(1, (most + CHUNK - 1) // CHUNK, more, 0)

    @pl.when(step == steps - 1)
    def _():
        stat_ref[0] = top_ref[...]
        stat_ref[1] = sum_ref[...]


def head_hist(q, w, e_all, tok_all, start, base, scale, nb=1280):
    cols = w.shape[1]
    n = e_all.shape[-1]
    whole = lambda *s: pl.BlockSpec(s, lambda i: (0,) * len(s), pipeline_mode=pl.Buffered(1))
    smem = pl.BlockSpec(memory_space=pltpu.SMEM)
    return pl.pallas_call(
        functools.partial(head_hist_kernel, nb // 256),
        grid=(cols // nb,),
        in_specs=[smem, smem, whole(32, 2048), pl.BlockSpec((2048, nb), lambda i: (0, i)), whole(8, 32, n), whole(8, 64, 128), whole(32, 256)],
        out_specs=[pl.BlockSpec((32, nb), lambda i: (0, i)), pl.BlockSpec((32, nb), lambda i: (0, i)), pl.BlockSpec((2, 32, 128), lambda i: (0, 0, 0))],
        out_shape=[jax.ShapeDtypeStruct((32, cols), F32), jax.ShapeDtypeStruct((32, cols), F32), jax.ShapeDtypeStruct((2, 32, 128), F32)],
        scratch_shapes=[pltpu.VMEM((32, 128), F32), pltpu.VMEM((32, 128), F32)],
        compiler_params=pltpu.CompilerParams(vmem_limit_bytes=VLIM),
        name="head_hist",
    )(start, base, q, w, e_all, tok_all, scale)


def stat_kernel(stat_ref, all_ref, ss, rs):
    s, m = lax.axis_index("store"), lax.axis_index("model")
    barrier = pltpu.get_barrier_semaphore()
    for j in range(1, 4):
        pl.semaphore_signal(barrier, inc=1, device_id=(0, s, lax.rem(m + j, 4)), device_id_type=MESH)
    pl.semaphore_wait(barrier, 3)
    out = [remote(stat_ref, all_ref.at[m], ss.at[j], rs.at[j], s, lax.rem(m + j, 4)) for j in range(1, 4)]
    for c in out:
        c.start()
    all_ref[m] = stat_ref[...]
    for c in out:
        c.wait()


def share_stats(stat):
    vm = pl.BlockSpec(memory_space=pltpu.VMEM)
    return pl.pallas_call(
        stat_kernel, in_specs=[vm], out_specs=vm, out_shape=jax.ShapeDtypeStruct((4, 2, 32, 128), F32),
        scratch_shapes=[pltpu.SemaphoreType.DMA((4,)), pltpu.SemaphoreType.DMA((4,))],
        compiler_params=pltpu.CompilerParams(collective_id=1, has_side_effects=True), name="share_stats",
    )(stat)


def mix_kernel(mix_ref, stat_ref, logit_ref, hist_ref, out_ref):
    tops, sums = stat_ref[:, 0], stat_ref[:, 1]
    top = jnp.max(tops, axis=0)
    total = jnp.sum(sums * jnp.exp(tops - top[None]), axis=0)
    share = ((1.0 - mix_ref[0, 0]) / total)[:, 0:1]
    out_ref[...] = jnp.log(hist_ref[...] + share * jnp.exp(logit_ref[...] - top[:, 0:1]))


def mix(lam, stats, logits, hist, nb=6400):
    rows, cols = logits.shape
    blk = pl.BlockSpec((rows, nb), lambda i: (0, i))
    return pl.pallas_call(
        mix_kernel, grid=(cols // nb,),
        in_specs=[pl.BlockSpec(memory_space=pltpu.SMEM), pl.BlockSpec((4, 2, 32, 128), lambda i: (0, 0, 0, 0)), blk, blk],
        out_specs=blk, out_shape=jax.ShapeDtypeStruct((rows, cols), F32), name="mix",
        compiler_params=pltpu.CompilerParams(vmem_limit_bytes=VLIM),
    )(lam, stats, logits, hist)


def solution(mesh):
    def local_step(queries, w_head, store_keys, store_tok, temperature, mix_weight):
        s, m = lax.axis_index("store"), lax.axis_index("model")
        me = s * 4 + m
        qt = jnp.concatenate([queries, queries], axis=0).T
        tau = temperature.reshape(1, 1)
        lam = mix_weight.reshape(1, 1)
        e, tok, start, stat = scores(qt, store_keys, store_tok.reshape(64, 128), tau)
        e_all, tok_all, start_all, stat_all = exchange(e, tok, start, stat)
        mine = lambda a, own: lax.dynamic_update_slice_in_dim(a, own[None], me, 0)
        e_all = mine(e_all, lax.dynamic_index_in_dim(e, s, 0, keepdims=False)).reshape(8, 32, -1)
        tok_all, start_all = mine(tok_all, tok), mine(start_all, start)
        stat_all = mine(stat_all, lax.dynamic_index_in_dim(stat, s, 0, keepdims=False))
        flat = start_all[:, :, :32].reshape(8, 1024)
        bounds = lax.dynamic_slice_in_dim(flat, m * 250, 251, 1)
        tops = stat_all[:, 0, :, 0]
        up = jnp.exp(tops - jnp.max(tops, axis=0))
        total = jnp.sum(up * stat_all[:, 1, :, 0], axis=0)
        scale = jnp.repeat((mix_weight * up / total).T, CHUNK, axis=1)
        rows = lax.dynamic_slice_in_dim(queries, s * 32, 32, 0)
        base = (m * 64000).astype(I32).reshape(1)
        logits, hist, lm = head_hist(rows, w_head, e_all, tok_all, bounds, base, scale)
        return mix(lam, share_stats(lm), logits, hist)

    group = ("store", "model")
    return jax.shard_map(local_step, mesh=mesh, in_specs=(P("data", None), P(None, "model"), P(group, None), P(group), P(), P()), out_specs=P(("data", "store"), "model"), check_vma=False)
```

```python
import functools

import jax
import jax.numpy as jnp
from jax import lax
from jax.experimental import pallas as pl
from jax.experimental.pallas import tpu as pltpu
from jax.sharding import PartitionSpec as P

MESH = pl.DeviceIdType.MESH
F32, BF16, I32 = jnp.float32, jnp.bfloat16, jnp.int32
VLIM = 60 * 1024 * 1024
CHUNK = 32


def iota(shape, dim):
    return lax.broadcasted_iota(I32, shape, dim)


def sort_rows(x):
    n = x.shape[0] * 128
    pos = iota(x.shape, 0) * 128 + iota(x.shape, 1)
    k = 2
    while k <= n:
        j = k // 2
        while j >= 1:
            if j >= 128:
                ahead, behind = pltpu.roll(x, 64 - j // 128, 0), pltpu.roll(x, j // 128, 0)
            else:
                ahead, behind = pltpu.roll(x, 128 - j, 1), pltpu.roll(x, j, 1)
            first = (pos & j) == 0
            other = jnp.where(first, ahead, behind)
            low = ((pos & k) == 0) == first
            x = jnp.where(low, jnp.minimum(x, other), jnp.maximum(x, other))
            j //= 2
        k *= 2
    return x


def score_kernel(qt_ref, keys_ref, tok_ref, tau_ref, e_ref, tok_out, start_out, stat_out, s_ref, top_ref, perm_v, perm_s, hot_a, hot_b, rows_ref, sem):
    step, steps = pl.program_id(0), pl.num_programs(0)
    kb = keys_ref.shape[0]
    sub = 256

    @pl.when(step == 0)
    def _():
        top_ref[...] = jnp.full_like(top_ref, -jnp.inf)
        tok = tok_ref[...]
        packed = sort_rows(tok * 8192 + (iota((64, 128), 0) * 128 + iota((64, 128), 1)))
        tok_out[...] = packed >> 13
        perm_v[...] = packed & 8191
        cp = pltpu.make_async_copy(perm_v, perm_s, sem)
        cp.start()
        for r in range(64):
            tile = tok_ref[r : r + 1, :] >> 8
            lanes = slice(r * 128, (r + 1) * 128)
            hot_a[:, lanes] = jnp.where(iota((32, 128), 0) == (tile >> 5), 1.0, 0.0).astype(BF16)
            hot_b[:, lanes] = jnp.where(iota((128, 128), 0) == (tile & 31), 1.0, 0.0).astype(BF16)
        cnt = lax.dot_general(hot_a[...], hot_b[...], (((1,), (1,)), ((), ())), preferred_element_type=F32)
        inc = cnt
        for sh in (1, 2, 4, 8, 16):
            inc = inc + jnp.where(iota((32, 128), 1) >= sh, pltpu.roll(inc, sh, 1), 0.0)
        tot = jnp.broadcast_to(jnp.sum(cnt, axis=1, keepdims=True), (32, 128))
        rp = tot
        for sh in (1, 2, 4, 8, 16):
            rp = rp + jnp.where(iota((32, 128), 0) >= sh, pltpu.roll(rp, sh, 0), 0.0)
        start_out[...] = ((inc - cnt) + (rp - tot)).astype(I32)
        cp.wait()

    def score(i, _):
        at = pl.multiple_of(i * sub, sub)
        kv = keys_ref[pl.ds(at, sub), :]
        dots = jnp.dot(kv, qt_ref[...], preferred_element_type=F32)
        kf = kv.astype(F32)
        norm = jnp.sum(kf * kf, axis=1, keepdims=True)
        s = (2.0 * dots - norm) / tau_ref[0, 0]
        s_ref[pl.ds(pl.multiple_of(step * kb + at, sub), sub), :] = s
        top_ref[...] = jnp.maximum(top_ref[...], jnp.max(s.reshape(sub // 8, 8, 128), axis=0))
        return 0

    lax.fori_loop(0, kb // sub, score, 0)

    @pl.when(step == steps - 1)
    def _():
        top = jnp.max(top_ref[...], axis=0, keepdims=True)

        def block(b, total):
            for u in range(128):
                rows_ref[u : u + 1, :] = s_ref[pl.ds(perm_s[b, u], 1), :]
            x = jnp.exp(rows_ref[...] - top)
            total = total + jnp.sum(x.reshape(16, 8, 128), axis=0)
            xt = x.T
            lanes = pl.ds(pl.multiple_of(b * 128, 128), 128)
            for g in range(8):
                e_ref[g // 4, g % 4, :, lanes] = xt[8 * g : 8 * g + 8, :]
            return total

        total = lax.fori_loop(0, 64, block, jnp.zeros((8, 128), F32))
        total = jnp.sum(total, axis=0, keepdims=True)
        mt = jnp.broadcast_to(top, (128, 128)).T
        zt = jnp.broadcast_to(total, (128, 128)).T
        for s in range(2):
            stat_out[s, 0] = mt[32 * s : 32 * s + 32]
            stat_out[s, 1] = zt[32 * s : 32 * s + 32]


def scores(qt, keys, tok, tau, kb=1024):
    n = keys.shape[0]
    whole = lambda *s: pl.BlockSpec(s, lambda i: (0,) * len(s))
    return pl.pallas_call(
        score_kernel,
        grid=(n // kb,),
        in_specs=[whole(2048, 128), pl.BlockSpec((kb, 2048), lambda i: (i, 0)), whole(64, 128), pl.BlockSpec(memory_space=pltpu.SMEM)],
        out_specs=[whole(2, 4, 8, n), whole(64, 128), whole(32, 128), whole(2, 2, 32, 128)],
        out_shape=[jax.ShapeDtypeStruct((2, 4, 8, n), F32), jax.ShapeDtypeStruct((64, 128), I32), jax.ShapeDtypeStruct((32, 128), I32), jax.ShapeDtypeStruct((2, 2, 32, 128), F32)],
        scratch_shapes=[
            pltpu.VMEM((n, 128), F32), pltpu.VMEM((8, 128), F32), pltpu.VMEM((64, 128), I32), pltpu.SMEM((64, 128), I32),
            pltpu.VMEM((32, n), BF16), pltpu.VMEM((128, n), BF16), pltpu.VMEM((128, 128), F32), pltpu.SemaphoreType.DMA,
        ],
        compiler_params=pltpu.CompilerParams(vmem_limit_bytes=VLIM),
        name="scores",
    )(qt, keys, tok, tau)


def peers():
    s, m = lax.axis_index("store"), lax.axis_index("model")
    x, c = m // 2, m % 2
    return s, m, 1 - s, (1 - x) * 2 + c, x * 2 + (1 - c)


def remote(src, dst, ss, rs, s, m):
    return pltpu.make_async_remote_copy(src_ref=src, dst_ref=dst, send_sem=ss, recv_sem=rs, device_id=(0, s, m), device_id_type=MESH)


def window(e_ref, tok_ref, starts, ends=None):
    lane, lane1 = iota((32, 128), 1), iota((1, 128), 1)
    halves, toks = [], []
    for h in range(2):
        acc, tacc = None, None
        for i in range(4):
            d = 4 * h + i
            at = starts[d]
            row, off = jnp.minimum(at >> 7, 63), at & 127
            nxt = jnp.minimum(row + 1, 63)
            v0 = e_ref[d, :, :, pl.ds(pl.multiple_of(row * 128, 128), 128)].reshape(32, 128)
            v1 = e_ref[d, :, :, pl.ds(pl.multiple_of(nxt * 128, 128), 128)].reshape(32, 128)
            sh = (CHUNK * i - off) & 127
            v = pltpu.roll(jnp.where(lane >= off, v0, v1), sh, 1)
            t0, t1 = tok_ref[d, pl.ds(row, 1), :], tok_ref[d, pl.ds(nxt, 1), :]
            t = pltpu.roll(jnp.where(lane1 >= off, t0, t1), sh, 1)
            if ends is not None:
                t = jnp.where(lane1 - CHUNK * i < ends[d] - at, t, -1)
            if i == 0:
                acc, tacc = v, t
            else:
                acc = jnp.where(lane >= CHUNK * i, v, acc)
                tacc = jnp.where(lane1 >= CHUNK * i, t, tacc)
        halves.append(acc)
        toks.append(tacc)
    return jnp.concatenate(halves, axis=1), jnp.concatenate(toks, axis=1)


def product(e, tok):
    hi = e.astype(BF16)
    rest = e - hi.astype(F32)
    mid = rest.astype(BF16)
    low = (rest - mid.astype(F32)).astype(BF16)
    lhs = jnp.concatenate([hi, mid, low], axis=0)
    hot = jnp.where(iota((256, 256), 0) == tok, 1.0, 0.0).astype(BF16)
    out = lax.dot_general(lhs, hot, (((1,), (1,)), ((), ())), preferred_element_type=F32)
    return out[0:32] + out[32:64] + out[64:96]


def source_scale(stat_ref, lam):
    tops = stat_ref[:, 0]
    up = jnp.exp(tops - jnp.max(tops, axis=0)[None])
    total = jnp.sum(up * stat_ref[:, 1], axis=0)
    up = up * (lam / total)[None]
    lane = iota((32, 128), 1)
    halves = []
    for h in range(2):
        acc = up[4 * h]
        for i in range(1, 4):
            acc = jnp.where(lane >= CHUNK * i, up[4 * h + i], acc)
        halves.append(acc)
    return jnp.concatenate(halves, axis=1)


NB = 512
NBUF = 10
TRIPS = 25
TILES = 10
PER = 2
WIDE = TILES * 256


class Head:
    def __init__(self, first, last, s, q_ref, w_ref, logit_ref, w_buf, l_buf, top_ref, sum_ref, w_sem, l_sem):
        self.__dict__.update({k: v for k, v in locals().items() if k != "self"})

    def w_copy(self, i):
        slot = lax.rem(i, NBUF)
        cols = pl.ds(pl.multiple_of((self.first + i) * NB, NB), NB)
        return pltpu.make_async_copy(self.w_ref.at[:, cols], self.w_buf.at[slot], self.w_sem.at[slot])

    def l_copy(self, i):
        slot = lax.rem(i, 2)
        cols = pl.ds(pl.multiple_of(i * NB, NB), NB)
        return pltpu.make_async_copy(self.l_buf.at[slot], self.logit_ref.at[:, cols], self.l_sem.at[slot])

    def prime(self):
        for i in range(NBUF - 2):
            self.w_copy(i).start()

    def enter(self, i):
        @pl.when(i + NBUF - 2 < self.last - self.first)
        def _():
            self.w_copy(i + NBUF - 2).start()

        @pl.when(i >= 2)
        def _():
            self.l_copy(i - 2).wait()

        self.w_copy(i).wait()

    def logits(self, i):
        out = jnp.dot(self.q_ref[self.s], self.w_buf[lax.rem(i, NBUF)], preferred_element_type=F32)
        self.l_buf[lax.rem(i, 2)] = out
        old = self.top_ref[...]
        new = jnp.maximum(old, jnp.max(out, axis=1, keepdims=True))
        self.sum_ref[...] = self.sum_ref[...] * jnp.exp(old - new) + jnp.sum(jnp.exp(out - new[:, 0:1]), axis=1, keepdims=True)
        self.top_ref[...] = new

    def drain(self):
        for i in (2, 1):
            self.l_copy(self.last - self.first - i).wait()

    def run(self, lo, hi):
        def one(i, _):
            self.enter(i)
            self.logits(i)
            self.l_copy(i).start()
            return 0

        lax.fori_loop(lo, hi, one, 0)


def head_scratch():
    dma = pltpu.SemaphoreType.DMA
    return [pltpu.VMEM((NBUF, 2048, NB), BF16), pltpu.VMEM((2, 32, NB), F32), pltpu.VMEM((32, 128), F32), pltpu.VMEM((32, 128), F32), dma((NBUF,)), dma((2,))]


def exchange_kernel(first, last, q_ref, e_ref, tok_ref, start_ref, stat_ref, w_ref,
                    logit_ref, e_all, tok_all, start_all, stat_all, lm_ref,
                    w_buf, l_buf, top_ref, sum_ref, w_sem, l_sem, loc_sem, es, er, ps, pr, ts, tr):
    s, m, so, mx, mc = peers()
    me = s * 4 + m
    head = Head(first, last, s, q_ref, w_ref, logit_ref, w_buf, l_buf, top_ref, sum_ref, w_sem, l_sem)
    head.prime()

    barrier = pltpu.get_barrier_semaphore()
    for j in range(1, 8):
        d = lax.rem(me + j, 8)
        pl.semaphore_signal(barrier, inc=1, device_id=(0, d // 4, lax.rem(d, 4)), device_id_type=MESH)
    pl.semaphore_wait(barrier, 7)

    far = []
    for r in range(4):
        far.append([
            remote(e_ref.at[so, r], e_all.at[me, r], es.at[0, r], er.at[0, r], so, mx),
            remote(e_ref.at[s, r], e_all.at[me, r], es.at[1, r], er.at[1, r], s, mx),
            remote(e_ref.at[so, r], e_all.at[me, r], es.at[2, r], er.at[2, r], so, m),
        ])
        for c in far[-1]:
            c.start()
    own = [remote(e_ref.at[s, r], e_all.at[me, r], ps.at[3, r], pr.at[3, r], s, mc) for r in range(4)]
    for c in own:
        c.start()
    small = []
    for j in range(1, 8):
        d = lax.rem(me + j, 8)
        ds_, dm = d // 4, lax.rem(d, 4)
        for k, (a, b) in enumerate(((tok_ref, tok_all.at[me]), (start_ref, start_all.at[me]), (stat_ref.at[ds_], stat_all.at[me]))):
            small.append(remote(a, b, ts.at[j, k], tr.at[j, k], ds_, dm))
    for c in small:
        c.start()
    mine = pltpu.make_async_copy(e_ref.at[s], e_all.at[me], loc_sem)
    mine.start()
    tok_all[me] = tok_ref[...]
    start_all[me] = start_ref[...]
    stat_all[me] = stat_ref[s]
    top_ref[...] = jnp.full_like(top_ref, -jnp.inf)
    sum_ref[...] = jnp.zeros_like(sum_ref)

    came = (so * 4 + mx, s * 4 + mx, so * 4 + m)
    blocks = last - first
    fwd = []
    for r in range(4):
        head.run(r * blocks // 4, (r + 1) * blocks // 4)
        for k in (1, 2, 0):
            far[r][k].wait_recv()
            f = remote(e_all.at[came[k], r], e_all.at[came[k], r], ps.at[k, r], pr.at[k, r], s, mc)
            f.start()
            fwd.append(f)
    head.drain()
    lm_ref[0] = top_ref[...]
    lm_ref[1] = sum_ref[...]
    mine.wait()
    for c in own + fwd + small:
        c.wait()
    for r in range(4):
        for c in far[r]:
            c.wait_send()


def exchange(first, last, q, e, tok, start, stat, w):
    n = e.shape[-1]
    anyspec, vm = pl.BlockSpec(memory_space=pl.ANY), pl.BlockSpec(memory_space=pltpu.VMEM)
    dma = pltpu.SemaphoreType.DMA
    return pl.pallas_call(
        functools.partial(exchange_kernel, first, last),
        in_specs=[vm, anyspec, vm, vm, vm, anyspec],
        out_specs=[anyspec, anyspec, vm, vm, vm, vm],
        out_shape=[
            jax.ShapeDtypeStruct((32, (last - first) * NB), F32), jax.ShapeDtypeStruct((8, 4, 8, n), F32),
            jax.ShapeDtypeStruct((8, 64, 128), I32), jax.ShapeDtypeStruct((8, 32, 128), I32), jax.ShapeDtypeStruct((8, 2, 32, 128), F32),
            jax.ShapeDtypeStruct((2, 32, 128), F32),
        ],
        scratch_shapes=head_scratch() + [dma, dma((3, 4)), dma((3, 4)), dma((4, 4)), dma((4, 4)), dma((8, 3)), dma((8, 3))],
        compiler_params=pltpu.CompilerParams(collective_id=0, has_side_effects=True, vmem_limit_bytes=VLIM),
        name="exchange",
    )(q, e, tok, start, stat, w)


def hist_kernel(first, last, pos_ref, lam_ref, start_s, q_ref, start_ref, tok_ref, stat_ref, lm_in, e_hbm, w_ref,
                logit_ref, hist_ref, lm_ref,
                e_ref, h_buf, scale_ref, wide_ref, h_sem, e_sem, w_buf, l_buf, top_ref, sum_ref, w_sem, l_sem):
    s, m = pos_ref[0], pos_ref[1]
    head = Head(first, last, s, q_ref, w_ref, logit_ref, w_buf, l_buf, top_ref, sum_ref, w_sem, l_sem)
    load = pltpu.make_async_copy(e_hbm, e_ref, e_sem)
    load.start()
    head.prime()
    top_ref[...] = lm_in[0]
    sum_ref[...] = lm_in[1]
    scale_ref[...] = source_scale(stat_ref, lam_ref[0, 0])
    low = m * (TRIPS * TILES)
    tile = iota((32, 128), 0) * 32 + iota((32, 128), 1)
    inside = (iota((32, 128), 1) < 32) & (tile >= low) & (tile < low + TRIPS * TILES)
    wide = jnp.zeros((32, 128), I32)
    for d in range(8):
        a = start_ref[d]
        below = jnp.broadcast_to(pltpu.roll(a, 31, 0)[:, 0:1], (32, 128))
        b = jnp.where(iota((32, 128), 1) == 31, below, pltpu.roll(a, 127, 1))
        wide = jnp.maximum(wide, jnp.where(inside, b - a, 0))
    wide_ref[0] = jnp.max(wide)
    load.wait()

    def h_copy(j):
        slot = lax.rem(j, 2)
        return pltpu.make_async_copy(h_buf.at[slot], hist_ref.at[:, pl.ds(pl.multiple_of(j * WIDE, 256), WIDE)], h_sem.at[slot])

    def edges(g):
        return [start_s[d, g >> 5, g & 31] for d in range(8)]

    def trip(j, _):
        for i in range(PER):
            head.enter(PER * j + i)

        @pl.when(j >= 2)
        def _():
            h_copy(j - 2).wait()

        slot = lax.rem(j, 2)
        scale = scale_ref[...]
        g0 = low + j * TILES
        for i in range(PER):
            head.logits(PER * j + i)
        for i in range(TILES):
            e, tok = window(e_ref, tok_ref, edges(g0 + i))
            h_buf[slot, :, i * 256 : (i + 1) * 256] = product(e * scale, tok - (g0 + i) * 256)
        for i in range(PER):
            head.l_copy(PER * j + i).start()

        @pl.when(wide_ref[0] > CHUNK)
        def _():
            def extra(i, _):
                starts, ends = edges(g0 + i), edges(g0 + i + 1)
                most = functools.reduce(jnp.maximum, [b - a for a, b in zip(starts, ends)])
                cols = pl.ds(pl.multiple_of(i * 256, 256), 256)

                def more(it, _):
                    at = [jnp.minimum(a + it * CHUNK, b) for a, b in zip(starts, ends)]
                    e, tok = window(e_ref, tok_ref, at, ends)
                    h_buf[slot, :, cols] += product(e * scale_ref[...], tok - (g0 + i) * 256)
                    return 0

                lax.fori_loop(1, (most + CHUNK - 1) // CHUNK, more, 0)
                return 0

            lax.fori_loop(0, TILES, extra, 0)

        h_copy(j).start()
        return 0

    lax.fori_loop(0, TRIPS, trip, 0)
    lm_ref[0] = top_ref[...]
    lm_ref[1] = sum_ref[...]
    head.drain()
    for i in (2, 1):
        h_copy(TRIPS - i).wait()


def hist_head(first, last, pos, lam, q, start, tok, stat, lm, e_all, w):
    cols = w.shape[1]
    anyspec, vm, sm = (pl.BlockSpec(memory_space=k) for k in (pl.ANY, pltpu.VMEM, pltpu.SMEM))
    dma = pltpu.SemaphoreType.DMA
    return pl.pallas_call(
        functools.partial(hist_kernel, first, last),
        in_specs=[sm, sm, sm, vm, vm, vm, vm, vm, anyspec, anyspec],
        out_specs=[anyspec, anyspec, vm],
        out_shape=[jax.ShapeDtypeStruct((32, (last - first) * NB), F32), jax.ShapeDtypeStruct((32, cols), F32), jax.ShapeDtypeStruct((2, 32, 128), F32)],
        scratch_shapes=[pltpu.VMEM(e_all.shape, F32), pltpu.VMEM((2, 32, WIDE), F32), pltpu.VMEM((32, 256), F32), pltpu.SMEM((1,), I32), dma((2,)), dma] + head_scratch(),
        compiler_params=pltpu.CompilerParams(vmem_limit_bytes=VLIM),
        name="hist_head",
    )(pos, lam, start, q, start, tok, stat, lm, e_all, w)


def stat_kernel(stat_ref, all_ref, ss, rs):
    s, m = lax.axis_index("store"), lax.axis_index("model")
    barrier = pltpu.get_barrier_semaphore()
    for j in range(1, 4):
        pl.semaphore_signal(barrier, inc=1, device_id=(0, s, lax.rem(m + j, 4)), device_id_type=MESH)
    pl.semaphore_wait(barrier, 3)
    out = [remote(stat_ref, all_ref.at[m], ss.at[j], rs.at[j], s, lax.rem(m + j, 4)) for j in range(1, 4)]
    for c in out:
        c.start()
    all_ref[m] = stat_ref[...]
    for c in out:
        c.wait()


def share_stats(stat):
    vm = pl.BlockSpec(memory_space=pltpu.VMEM)
    return pl.pallas_call(
        stat_kernel, in_specs=[vm], out_specs=vm, out_shape=jax.ShapeDtypeStruct((4, 2, 32, 128), F32),
        scratch_shapes=[pltpu.SemaphoreType.DMA((4,)), pltpu.SemaphoreType.DMA((4,))],
        compiler_params=pltpu.CompilerParams(collective_id=1, has_side_effects=True), name="share_stats",
    )(stat)


def mix_kernel(cuts, lam_ref, stat_ref, *refs):
    parts, hist_ref, out_ref = refs[:-2], refs[-2], refs[-1]
    tops, sums = stat_ref[:, 0], stat_ref[:, 1]
    top = jnp.max(tops, axis=0)
    total = jnp.sum(sums * jnp.exp(tops - top[None]), axis=0)
    share = ((1.0 - lam_ref[0, 0]) / total)[:, 0:1]
    step = pl.program_id(0)
    for k, ref in enumerate(parts):
        @pl.when((step >= cuts[k]) & (step < cuts[k + 1]))
        def _():
            out_ref[...] = jnp.log(hist_ref[...] + share * jnp.exp(ref[...] - top[:, 0:1]))


def mix(lam, stats, parts, hist, nb=6400):
    rows, cols = hist.shape
    blk = pl.BlockSpec((rows, nb), lambda i: (0, i))
    cuts = [0]
    for p in parts:
        cuts.append(cuts[-1] + p.shape[1] // nb)
    part = lambda k: pl.BlockSpec((rows, nb), lambda i: (0, jnp.clip(i - cuts[k], 0, cuts[k + 1] - cuts[k] - 1)))
    return pl.pallas_call(
        functools.partial(mix_kernel, tuple(cuts)), grid=(cols // nb,),
        in_specs=[pl.BlockSpec(memory_space=pltpu.SMEM), pl.BlockSpec((4, 2, 32, 128), lambda i: (0, 0, 0, 0))] + [part(k) for k in range(len(parts))] + [blk],
        out_specs=blk, out_shape=jax.ShapeDtypeStruct((rows, cols), F32), name="mix",
        compiler_params=pltpu.CompilerParams(vmem_limit_bytes=VLIM),
    )(lam, stats, *parts, hist)


def solution(mesh):
    def local_step(queries, w_head, store_keys, store_tok, temperature, mix_weight):
        s, m = lax.axis_index("store"), lax.axis_index("model")
        blocks = w_head.shape[1] // NB
        cut = blocks - PER * TRIPS
        qt = jnp.concatenate([queries, queries], axis=0).T
        tau = temperature.reshape(1, 1)
        lam = mix_weight.reshape(1, 1)
        q = queries.reshape(2, 32, -1)
        e, tok, start, stat = scores(qt, store_keys, store_tok.reshape(64, 128), tau)
        la, e_all, tok_all, start_all, stat_all, lm = exchange(0, cut, q, e, tok, start, stat, w_head)
        pos = jnp.stack([s, m]).astype(I32)
        lb, hist, lm = hist_head(cut, blocks, pos, lam, q, start_all, tok_all, stat_all, lm, e_all, w_head)
        return mix(lam, share_stats(lm), [la, lb], hist)

    group = ("store", "model")
    return jax.shard_map(local_step, mesh=mesh, in_specs=(P("data", None), P(None, "model"), P(group, None), P(group), P(), P()), out_specs=P(("data", "store"), "model"), check_vma=False)
```
